32 devices in a mesh: row: 4 (over x, core), col: 8 (over z, y).
Axes of the slice: x: 2, y: 2, z: 4, core: 2. Of those that a mesh axis runs over, the one named last changes fastest.
Arguments:
- normed: bfloat16 [12288, 6144], P(('row', 'col')), may hold values from -6 to 6
- out_grad: bfloat16 [12288, 6144], P(('row', 'col')), may hold values from -0.125 to 0.125
- w_in: bfloat16 [6144, 48], replicated, may hold values from -0.078125 to 0.078125
- hidden_grad: bfloat16 [12288, 48], P(('row', 'col')), may hold values from -0.125 to 0.125
- qkv_grad: bfloat16 [12288, 64], P(('row', 'col')), may hold values from -0.125 to 0.125
- bucket_order: int32 [160], replicated, may hold values from 0 to 159, each once
Outputs:
- buckets: bfloat16 [160, 6144], replicated
The draws below stay inside these ranges and needn't reach their ends.
Inputs may be any that keep to these rules, and one draw needn't show every extreme that they name: bucket_order is a permutation of 0 to 159.
All inputs are finite; a program needn't handle non-finite values.
Results may differ from the reference program's by a relative error of at most 0.0044.
Values may be sent and summed in bfloat16 or wider, within the bound.
A program may use at most 64 MiB of HBM per device.

```python
import jax
import jax.numpy as jnp
from jax import lax

D = 6144
QW = 64
HW = 48
TOK_DEV = 384
TOKENS = 12288
N_ROW = 4
N_COL = 8


def steps_of(own_key, shape, pieces, low, high):
    gain, own = 1.0, jax.random.fold_in(own_key, 6)
    for dim, shards_of in pieces:
        heights = jnp.exp(jax.random.uniform(jax.random.fold_in(own, dim), (shards_of,), jnp.float32, low / len(pieces), high / len(pieces)))
        gain = gain * jnp.repeat(heights, shape[dim] // shards_of).reshape([-1 if axis == dim else 1 for axis in range(len(shape))])
    return gain


def bell_draw(own_key, extent, scale, limit, cuts=(), held_as=jnp.bfloat16):
    values = jax.random.normal(own_key, extent, jnp.float32) * scale
    if len(cuts) > 0:
        values = steps_of(own_key, extent, cuts, -0.22, 0.18) * values
    return jnp.clip(values, min=-limit, max=limit).astype(held_as)


def setup_inputs(seed: int = 0) -> dict:
    seeds = jax.random.split(jax.random.key(seed), 7)
    normed = bell_draw(seeds[0], (TOKENS, D), 1.0, 6.0, ((0, 32),))
    out_grad = bell_draw(seeds[1], (TOKENS, D), ((TOK_DEV * N_ROW * N_COL) ** -0.5), 0.125, ((0, 32),))
    w_in = bell_draw(seeds[2], (D, HW), D ** -0.5, 0.078125)
    hidden_grad = bell_draw(seeds[3], (TOKENS, HW), ((TOK_DEV * N_ROW * N_COL) ** -0.5), 0.125, ((0, 32),))
    qkv_grad = bell_draw(seeds[4], (TOKENS, QW), ((TOK_DEV * N_ROW * N_COL) ** -0.5), 0.125, ((0, 32),))
    bucket_order = jax.random.permutation(seeds[5], QW + 2 * HW).astype(jnp.int32)
    return {"normed": normed, "out_grad": out_grad, "w_in": w_in, "hidden_grad": hidden_grad, "qkv_grad": qkv_grad, "bucket_order": bucket_order}


def reference(normed, out_grad, w_in, hidden_grad, qkv_grad, bucket_order):
    pre = jnp.dot(normed, w_in, preferred_element_type=jnp.float32)
    cdf = 0.5 * (1.0 + lax.erf(pre * 0.7071067811865476))
    pdf = jnp.exp(-0.5 * pre * pre) * 0.3989422804014327
    hidden = (pre * cdf).astype(jnp.bfloat16)
    pre_grad = (hidden_grad.astype(jnp.float32) * (cdf + pre * pdf)).astype(jnp.bfloat16)
    grad_qkv = jnp.dot(qkv_grad.T, normed, preferred_element_type=jnp.float32)
    grad_in = jnp.dot(pre_grad.T, normed, preferred_element_type=jnp.float32)
    grad_out = jnp.dot(hidden.T, out_grad, preferred_element_type=jnp.float32)
    stacked = jnp.concatenate([grad_qkv, grad_in, grad_out], axis=0)
    return jnp.take(stacked, bucket_order.astype(jnp.int32), axis=0).astype(jnp.bfloat16)
```

```python
import functools

import jax
import jax.numpy as jnp
from jax import lax
from jax.experimental import pallas as pl
from jax.experimental.pallas import tpu as pltpu
from jax.sharding import PartitionSpec as P

MESH = pl.DeviceIdType.MESH
LAG = 2
F32, BF16 = jnp.float32, jnp.bfloat16


def round_up(a, b):
    return -(-a // b) * b


def plan(n_row, n_col, d, qw, hw):
    nx, nz = n_row // 2, 4
    ny = n_col // nz
    unit = 2 * ny * nz * 128
    dp = round_up(d, unit)
    chunks = dp // unit
    rows = (round_up(qw, 16 * nx), round_up(2 * hw, 16 * nx))
    return dict(nx=nx, ny=ny, nz=nz, dp=dp, t=chunks, rows=rows, ch=ny * nz * 128, cy=nz * 128, cz=128, qw=qw, hw=hw)


def kernel(p, normed, out_grad, w_in, hidden_grad, qkv_grad, out, nrm, ogr, in_sem, out_sem, own, snd0, rcv0, s1, s2q, s2m, s3, ra_q, ra_m, rb_q, rb_m, rc, acc_q, acc_m, acc2, obuf, ssem, rsem):
    nx, ny, nz, nt = p["nx"], p["ny"], p["nz"], p["t"]
    ch, cy, cz = p["ch"], p["cy"], p["cz"]
    qw, hw = p["qw"], p["hw"]
    rows = p["rows"]
    base = (0, rows[0])
    part = (rows[0] // nx, rows[1] // nx)
    ct = 2 * ch
    r, c = lax.axis_index("row"), lax.axis_index("col")
    ic, ix = lax.rem(r, 2), r // 2
    iy, iz = lax.rem(c, ny), c // ny
    partner = (ix * 2 + (1 - ic), c)
    xp = [(lax.rem(ix + d, nx) * 2 + ic, c) for d in range(nx)]
    yp = [(r, iz * ny + lax.rem(iy + d, ny)) for d in range(ny)]
    zp = [(r, lax.rem(iz + d, nz) * ny + iy) for d in range(nz)]

    loads = {}
    for name, src, dst in (("n", normed, nrm), ("o", out_grad, ogr)):
        for t in range(nt):
            cols = pl.ds(t * ct, ct)
            cp = pltpu.make_async_copy(src.at[:, cols], dst.at[:, cols], in_sem.at[len(loads)])
            cp.start()
            loads[name, t] = cp

    barrier = pltpu.get_barrier_semaphore()
    peers = [partner] + xp[1:] + yp[1:] + zp[1:]
    for dev in peers:
        pl.semaphore_signal(barrier, inc=1, device_id=dev, device_id_type=MESH)

    lhs_q = qkv_grad[...].astype(F32).T.astype(BF16)

    sent = []

    def send(src, dst, dev):
        i = len(sent)
        cp = pltpu.make_async_remote_copy(src_ref=src, dst_ref=dst, send_sem=ssem.at[i], recv_sem=rsem.at[i], device_id=dev, device_id_type=MESH)
        cp.start()
        sent.append(cp)
        return cp

    def m(v, k):
        return pl.multiple_of(v, k)

    other_off = m((1 - ic) * ch, 128)
    own_off = m(ic * ch, 128)
    flight = {}

    def dot(lhs, buf, off):
        return jnp.dot(lhs, buf[:, pl.ds(off, ch)], preferred_element_type=F32)

    def zero_tail(g, used, dst, cols):
        if rows[g] > used:
            dst[pl.ds(base[g] + used, rows[g] - used), cols] = jnp.zeros((rows[g] - used, ch), F32)

    def ship(g, t):
        region = (pl.ds(base[g], rows[g]), pl.ds(t * ch, ch))
        flight[g, t, 0] = [send(snd0.at[region], rcv0.at[region], partner)]

    pre = None

    def partial_q(t):
        cols = pl.ds(t * ch, ch)
        snd0[pl.ds(0, qw), cols] = dot(lhs_q, nrm, m(t * ct + other_off, 128))
        zero_tail(0, qw, snd0, cols)
        ship(0, t)
        own[pl.ds(0, qw), cols] = dot(lhs_q, nrm, m(t * ct + own_off, 128))
        zero_tail(0, qw, own, cols)

    def partial_m(t):
        cols = pl.ds(t * ch, ch)
        for dst, off in ((snd0, other_off), (own, own_off)):
            at = m(t * ct + off, 128)
            dst[pl.ds(base[1], hw), cols] = dot(lhs_in, nrm, at)
            dst[pl.ds(base[1] + hw, hw), cols] = dot(lhs_out, ogr, at)
            zero_tail(1, 2 * hw, dst, cols)
            if dst is snd0:
                ship(1, t)

    def wait(g, t, s):
        for cp in flight[g, t, s]:
            cp.wait_recv()

    def row_part(g, i):
        return pl.ds(m(i * part[g], 16), part[g])

    def stage1(g, t):
        wait(g, t, 0)
        region = (pl.ds(base[g], rows[g]), pl.ds(t * ch, ch))
        v = own[region] + rcv0[region]
        own[region] = v
        s1[region] = v.astype(BF16)
        cps = []
        if g == 0:
            for d in range(1, nx):
                src = s1.at[row_part(0, lax.rem(ix + d, nx)), pl.ds(t * ch, ch)]
                cps.append(send(src, ra_q.at[d - 1, :, pl.ds(t * ch, ch)], xp[d]))
        else:
            for d in range(1, ny):
                src = s1.at[pl.ds(base[1], rows[1]), pl.ds(m(t * ch + lax.rem(iy + d, ny) * cy, 128), cy)]
                cps.append(send(src, ra_m.at[d - 1, :, pl.ds(t * cy, cy)], yp[d]))
        flight[g, t, 1] = cps

    def stage2(g, t):
        wait(g, t, 1)
        cps = []
        if g == 0:
            cols = pl.ds(t * ch, ch)
            v = own[row_part(0, ix), cols]
            for d in range(1, nx):
                v = v + ra_q[d - 1, :, cols].astype(F32)
            acc_q[:, cols] = v
            s2q[:, cols] = v.astype(BF16)
            for d in range(1, ny):
                src = s2q.at[:, pl.ds(m(t * ch + lax.rem(iy + d, ny) * cy, 128), cy)]
                cps.append(send(src, rb_q.at[d - 1, :, pl.ds(t * cy, cy)], yp[d]))
        else:
            cols = pl.ds(t * cy, cy)
            v = own[pl.ds(base[1], rows[1]), pl.ds(m(t * ch + iy * cy, 128), cy)]
            for d in range(1, ny):
                v = v + ra_m[d - 1, :, cols].astype(F32)
            acc_m[:, cols] = v
            s2m[:, cols] = v.astype(BF16)
            for d in range(1, nx):
                src = s2m.at[row_part(1, lax.rem(ix + d, nx)), cols]
                cps.append(send(src, rb_m.at[d - 1, :, cols], xp[d]))
        flight[g, t, 2] = cps

    def stage3(g, t):
        wait(g, t, 2)
        cols = pl.ds(t * cy, cy)
        at = pl.ds(g * part[0], part[g])
        if g == 0:
            v = acc_q[:, pl.ds(m(t * ch + iy * cy, 128), cy)]
            for d in range(1, ny):
                v = v + rb_q[d - 1, :, cols].astype(F32)
        else:
            v = acc_m[row_part(1, ix), cols]
            for d in range(1, nx):
                v = v + rb_m[d - 1, :, cols].astype(F32)
        acc2[at, cols] = v
        s3[at, cols] = v.astype(BF16)
        cps = []
        for d in range(1, nz):
            src = s3.at[at, pl.ds(m(t * cy + lax.rem(iz + d, nz) * cz, 128), cz)]
            cps.append(send(src, rc.at[d - 1, at, pl.ds(t * cz, cz)], zp[d]))
        flight[g, t, 3] = cps

    def mine(g):
        return pl.ds(m(base[g] + ix * part[g], 16), part[g])

    def spread(region, devs):
        return [send(obuf.at[region], obuf.at[region], dev) for dev in devs]

    def stage4(g, t):
        wait(g, t, 3)
        at = pl.ds(g * part[0], part[g])
        v = acc2[at, pl.ds(m(t * cy + iz * cz, 128), cz)]
        for d in range(1, nz):
            v = v + rc[d - 1, at, pl.ds(t * cz, cz)].astype(F32)
        region = (mine(g), pl.ds(m(t * ct + own_off + iy * cy + iz * cz, 128), cz))
        obuf[region] = v.astype(BF16)
        flight[g, t, 4] = spread(region, zp[1:])

    def stage5(g, t):
        wait(g, t, 4)
        region = (mine(g), pl.ds(m(t * ct + own_off + iy * cy, 128), cy))
        flight[g, t, 5] = spread(region, (yp if g == 0 else xp)[1:])

    def stage6(g, t):
        wait(g, t, 5)
        if g == 0:
            flight[g, t, 6] = spread((mine(0), pl.ds(m(t * ct + own_off, 128), ch)), xp[1:])
        else:
            flight[g, t, 6] = spread((pl.ds(base[1], rows[1]), pl.ds(m(t * ct + own_off + iy * cy, 128), cy)), yp[1:])

    def stage7(g, t):
        wait(g, t, 6)
        flight[g, t, 7] = spread((pl.ds(base[g], rows[g]), pl.ds(m(t * ct + own_off, 128), ch)), [partner])

    outs = []

    def stage8(g, t):
        wait(g, t, 7)
        region = (pl.ds(base[g], rows[g]), pl.ds(t * ct, ct))
        cp = pltpu.make_async_copy(obuf.at[region], out.at[region], out_sem.at[g * nt + t])
        cp.start()
        outs.append(cp)

    stages = [None, stage1, stage2, stage3, stage4, stage5, stage6, stage7, stage8]

    for t in range(nt):
        loads["n", t].wait()
        if t == 0:
            pl.semaphore_wait(barrier, len(peers))
        partial_q(t)
        term = jnp.dot(nrm[:, t * ct : (t + 1) * ct], w_in[t * ct : (t + 1) * ct, :], preferred_element_type=F32)
        pre = term if pre is None else pre + term
    for t in range(nt):
        stage1(0, t)
    cdf = 0.5 * (1.0 + lax.erf(pre * 0.7071067811865476))
    pdf = jnp.exp(-0.5 * pre * pre) * 0.3989422804014327
    lhs_out = (pre * cdf).T.astype(BF16)
    lhs_in = (hidden_grad[...].astype(F32) * (cdf + pre * pdf)).T.astype(BF16)
    for t in range(nt):
        loads["o", t].wait()
        partial_m(t)
    for step in range(2, 9 + LAG):
        for t in range(nt):
            if step <= 8:
                stages[step](0, t)
            if 1 <= step - LAG + 1 <= 8:
                stages[step - LAG + 1](1, t)
    for cp in sent:
        cp.wait_send()
    for cp in outs:
        cp.wait()


def local(p, normed, out_grad, w_in, hidden_grad, qkv_grad, bucket_order):
    tok, d = normed.shape
    dp, nt, nx, ny, nz = p["dp"], p["t"], p["nx"], p["ny"], p["nz"]
    ch, cy, cz, rows = p["ch"], p["cy"], p["cz"], p["rows"]
    if dp > d:
        normed = jnp.pad(normed, ((0, 0), (0, dp - d)))
        out_grad = jnp.pad(out_grad, ((0, 0), (0, dp - d)))
        w_in = jnp.pad(w_in, ((0, dp - d), (0, 0)))
    total = sum(rows)
    part = (rows[0] // nx, rows[1] // nx)
    per_chunk = 2 + 2 * (nx - 1) + 2 * (ny - 1) + 2 * (nz - 1)
    copies = 2 * nt * per_chunk
    vmem = pl.BlockSpec(memory_space=pltpu.VMEM)
    hbm = pl.BlockSpec(memory_space=pl.ANY)
    gathered = pl.pallas_call(
        functools.partial(kernel, p),
        out_shape=jax.ShapeDtypeStruct((total, dp), BF16),
        in_specs=[hbm, hbm, vmem, vmem, vmem],
        out_specs=hbm,
        scratch_shapes=[
            pltpu.VMEM((tok, dp), BF16),
            pltpu.VMEM((tok, dp), BF16),
            pltpu.SemaphoreType.DMA((2 * nt,)),
            pltpu.SemaphoreType.DMA((2 * nt,)),
            pltpu.VMEM((total, nt * ch), F32),
            pltpu.VMEM((total, nt * ch), F32),
            pltpu.VMEM((total, nt * ch), F32),
            pltpu.VMEM((total, nt * ch), BF16),
            pltpu.VMEM((part[0], nt * ch), BF16),
            pltpu.VMEM((rows[1], nt * cy), BF16),
            pltpu.VMEM((sum(part), nt * cy), BF16),
            pltpu.VMEM((nx - 1, part[0], nt * ch), BF16),
            pltpu.VMEM((ny - 1, rows[1], nt * cy), BF16),
            pltpu.VMEM((ny - 1, part[0], nt * cy), BF16),
            pltpu.VMEM((nx - 1, part[1], nt * cy), BF16),
            pltpu.VMEM((nz - 1, sum(part), nt * cz), BF16),
            pltpu.VMEM((part[0], nt * ch), F32),
            pltpu.VMEM((rows[1], nt * cy), F32),
            pltpu.VMEM((sum(part), nt * cy), F32),
            pltpu.VMEM((total, dp), BF16),
            pltpu.SemaphoreType.DMA((copies,)),
            pltpu.SemaphoreType.DMA((copies,)),
        ],
        compiler_params=pltpu.CompilerParams(collective_id=0, has_side_effects=True, vmem_limit_bytes=60 * 2**20),
    )(normed, out_grad, w_in, hidden_grad, qkv_grad)
    order = jnp.where(bucket_order < p["qw"], bucket_order, bucket_order + (rows[0] - p["qw"]))
    pick = (order[:, None] == jnp.arange(total, dtype=jnp.int32)[None, :]).astype(BF16)
    return jnp.dot(pick, gathered[:, :d], preferred_element_type=F32).astype(BF16)


def solution(mesh):
    n_row, n_col = mesh.shape["row"], mesh.shape["col"]
    split = P(("row", "col"), None)

    def step(normed, out_grad, w_in, hidden_grad, qkv_grad, bucket_order):
        p = plan(n_row, n_col, normed.shape[1], qkv_grad.shape[1], w_in.shape[1])
        body = jax.shard_map(
            functools.partial(local, p),
            mesh=mesh,
            in_specs=(split, split, P(), split, split, P()),
            out_specs=P(),
            check_vma=False,
        )
        return body(normed, out_grad, w_in, hidden_grad, qkv_grad, bucket_order)

    return step
```

```python
import functools

import jax
import jax.numpy as jnp
from jax import lax
from jax.experimental import pallas as pl
from jax.experimental.pallas import tpu as pltpu
from jax.sharding import PartitionSpec as P

MESH = pl.DeviceIdType.MESH
LAG = 0
F32, BF16 = jnp.float32, jnp.bfloat16


def round_up(a, b):
    return -(-a // b) * b


def plan(n_row, n_col, d, qw, hw):
    nx, nz = n_row // 2, 4
    ny = n_col // nz
    unit = 2 * ny * nz * 128
    dp = round_up(d, unit)
    chunks = dp // unit
    rows = (round_up(qw, 16 * nx), round_up(2 * hw, 16 * nx))
    return dict(nx=nx, ny=ny, nz=nz, dp=dp, t=chunks, rows=rows, ch=ny * nz * 128, cy=nz * 128, cz=128, qw=qw, hw=hw)


def kernel(p, normed, out_grad, w_hbm, hidden_hbm, qkv_hbm, out, nrm, ogr, w_in, hidden_grad, qkv_grad, in_sem, out_sem, own, snd0, rcv0, s1, s2q, s2m, s3, ra_q, ra_m, rb_q, rb_m, rc, acc_q, acc_m, acc2, obuf, ssem, rsem):
    nx, ny, nz, nt = p["nx"], p["ny"], p["nz"], p["t"]
    ch, cy, cz = p["ch"], p["cy"], p["cz"]
    qw, hw = p["qw"], p["hw"]
    rows = p["rows"]
    base = (0, rows[0])
    part = (rows[0] // nx, rows[1] // nx)
    ct = 2 * ch
    r, c = lax.axis_index("row"), lax.axis_index("col")
    ic, ix = lax.rem(r, 2), r // 2
    iy, iz = lax.rem(c, ny), c // ny
    partner = (ix * 2 + (1 - ic), c)
    xp = [(lax.rem(ix + d, nx) * 2 + ic, c) for d in range(nx)]
    yp = [(r, iz * ny + lax.rem(iy + d, ny)) for d in range(ny)]
    zp = [(r, lax.rem(iz + d, nz) * ny + iy) for d in range(nz)]

    loads = {}

    def load(key, src, dst):
        loads[key] = pltpu.make_async_copy(src, dst, in_sem.at[len(loads)])
        loads[key].start()

    def load_cols(name, src, dst, t):
        cols = pl.ds(t * ct, ct)
        load((name, t), src.at[:, cols], dst.at[:, cols])

    load("w", w_hbm, w_in)
    for t in range(nt):
        load_cols("n", normed, nrm, t)
    load("h", hidden_hbm, hidden_grad)
    load("q", qkv_hbm, qkv_grad)
    barrier = pltpu.get_barrier_semaphore()
    peers = [partner] + xp[1:] + yp[1:] + zp[1:]
    for dev in peers:
        pl.semaphore_signal(barrier, inc=1, device_id=dev, device_id_type=MESH)


    sent = []

    def send(src, dst, dev):
        i = len(sent)
        cp = pltpu.make_async_remote_copy(src_ref=src, dst_ref=dst, send_sem=ssem.at[i], recv_sem=rsem.at[i], device_id=dev, device_id_type=MESH)
        cp.start()
        sent.append(cp)
        return cp

    def m(v, k):
        return pl.multiple_of(v, k)

    other_off = m((1 - ic) * ch, 128)
    own_off = m(ic * ch, 128)
    flight = {}

    def dot(lhs, buf, off):
        return jnp.dot(lhs, buf[:, pl.ds(off, ch)], preferred_element_type=F32)

    def zero_tail(g, used, dst, cols):
        if rows[g] > used:
            dst[pl.ds(base[g] + used, rows[g] - used), cols] = jnp.zeros((rows[g] - used, ch), F32)

    def ship(g, t):
        region = (pl.ds(base[g], rows[g]), pl.ds(t * ch, ch))
        flight[g, t, 0] = [send(snd0.at[region], rcv0.at[region], partner)]

    def partial(dst, off, t):
        cols = pl.ds(t * ch, ch)
        at = m(t * ct + off, 128)
        v = dot(lhs_n, nrm, at)
        dst[pl.ds(0, qw), cols] = v[:qw]
        dst[pl.ds(base[1], hw), cols] = v[qw:]
        dst[pl.ds(base[1] + hw, hw), cols] = dot(lhs_out, ogr, at)
        zero_tail(0, qw, dst, cols)
        zero_tail(1, 2 * hw, dst, cols)

    def wait(g, t, s):
        for cp in flight[g, t, s]:
            cp.wait_recv()

    def row_part(g, i):
        return pl.ds(m(i * part[g], 16), part[g])

    def stage1(g, t):
        wait(g, t, 0)
        region = (pl.ds(base[g], rows[g]), pl.ds(t * ch, ch))
        v = own[region] + rcv0[region]
        own[region] = v
        s1[region] = v.astype(BF16)
        cps = []
        if g == 0:
            for d in range(1, nx):
                src = s1.at[row_part(0, lax.rem(ix + d, nx)), pl.ds(t * ch, ch)]
                cps.append(send(src, ra_q.at[d - 1, :, pl.ds(t * ch, ch)], xp[d]))
        else:
            for d in range(1, ny):
                src = s1.at[pl.ds(base[1], rows[1]), pl.ds(m(t * ch + lax.rem(iy + d, ny) * cy, 128), cy)]
                cps.append(send(src, ra_m.at[d - 1, :, pl.ds(t * cy, cy)], yp[d]))
        flight[g, t, 1] = cps

    def stage2(g, t):
        wait(g, t, 1)
        cps = []
        if g == 0:
            cols = pl.ds(t * ch, ch)
            v = own[row_part(0, ix), cols]
            for d in range(1, nx):
                v = v + ra_q[d - 1, :, cols].astype(F32)
            acc_q[:, cols] = v
            s2q[:, cols] = v.astype(BF16)
            for d in range(1, ny):
                src = s2q.at[:, pl.ds(m(t * ch + lax.rem(iy + d, ny) * cy, 128), cy)]
                cps.append(send(src, rb_q.at[d - 1, :, pl.ds(t * cy, cy)], yp[d]))
        else:
            cols = pl.ds(t * cy, cy)
            v = own[pl.ds(base[1], rows[1]), pl.ds(m(t * ch + iy * cy, 128), cy)]
            for d in range(1, ny):
                v = v + ra_m[d - 1, :, cols].astype(F32)
            acc_m[:, cols] = v
            s2m[:, cols] = v.astype(BF16)
            for d in range(1, nx):
                src = s2m.at[row_part(1, lax.rem(ix + d, nx)), cols]
                cps.append(send(src, rb_m.at[d - 1, :, cols], xp[d]))
        flight[g, t, 2] = cps

    def stage3(g, t):
        wait(g, t, 2)
        cols = pl.ds(t * cy, cy)
        at = pl.ds(g * part[0], part[g])
        if g == 0:
            v = acc_q[:, pl.ds(m(t * ch + iy * cy, 128), cy)]
            for d in range(1, ny):
                v = v + rb_q[d - 1, :, cols].astype(F32)
        else:
            v = acc_m[row_part(1, ix), cols]
            for d in range(1, nx):
                v = v + rb_m[d - 1, :, cols].astype(F32)
        acc2[at, cols] = v
        s3[at, cols] = v.astype(BF16)
        cps = []
        for d in range(1, nz):
            src = s3.at[at, pl.ds(m(t * cy + lax.rem(iz + d, nz) * cz, 128), cz)]
            cps.append(send(src, rc.at[d - 1, at, pl.ds(t * cz, cz)], zp[d]))
        flight[g, t, 3] = cps

    def mine(g):
        return pl.ds(m(base[g] + ix * part[g], 16), part[g])

    def spread(region, devs):
        return [send(obuf.at[region], obuf.at[region], dev) for dev in devs]

    def stage4(g, t):
        wait(g, t, 3)
        at = pl.ds(g * part[0], part[g])
        v = acc2[at, pl.ds(m(t * cy + iz * cz, 128), cz)]
        for d in range(1, nz):
            v = v + rc[d - 1, at, pl.ds(t * cz, cz)].astype(F32)
        region = (mine(g), pl.ds(m(t * ct + own_off + iy * cy + iz * cz, 128), cz))
        obuf[region] = v.astype(BF16)
        flight[g, t, 4] = spread(region, zp[1:])

    def stage5(g, t):
        wait(g, t, 4)
        region = (mine(g), pl.ds(m(t * ct + own_off + iy * cy, 128), cy))
        flight[g, t, 5] = spread(region, (yp if g == 0 else xp)[1:])

    def stage6(g, t):
        wait(g, t, 5)
        if g == 0:
            flight[g, t, 6] = spread((mine(0), pl.ds(m(t * ct + own_off, 128), ch)), xp[1:])
        else:
            flight[g, t, 6] = spread((pl.ds(base[1], rows[1]), pl.ds(m(t * ct + own_off + iy * cy, 128), cy)), yp[1:])

    def stage7(g, t):
        wait(g, t, 6)
        flight[g, t, 7] = spread((pl.ds(base[g], rows[g]), pl.ds(m(t * ct + own_off, 128), ch)), [partner])

    outs = []

    def stage8(g, t):
        wait(g, t, 7)
        region = (pl.ds(base[g], rows[g]), pl.ds(t * ct, ct))
        cp = pltpu.make_async_copy(obuf.at[region], out.at[region], out_sem.at[g * nt + t])
        cp.start()
        outs.append(cp)

    stages = [None, stage1, stage2, stage3, stage4, stage5, stage6, stage7, stage8]

    pre = None
    for t in range(nt):
        loads["n", t].wait()
        if t == 0:
            loads["w"].wait()
        load_cols("o", out_grad, ogr, t)
        cols = slice(t * ct, (t + 1) * ct)
        term = lax.dot_general(w_in[:, cols], nrm[:, cols], (((1,), (1,)), ((), ())), preferred_element_type=F32)
        pre = term if pre is None else pre + term
    loads["h"].wait()
    loads["q"].wait()
    lhs_q = qkv_grad[...]
    cdf = 0.5 * (1.0 + lax.erf(pre * 0.7071067811865476))
    pdf = jnp.exp(-0.5 * pre * pre) * 0.3989422804014327
    lhs_out = (pre * cdf).astype(BF16)
    lhs_in = (hidden_grad[...].astype(F32) * (cdf + pre * pdf)).astype(BF16)
    lhs_n = jnp.concatenate([lhs_q, lhs_in], axis=0)
    pl.semaphore_wait(barrier, len(peers))
    for t in range(nt):
        loads["o", t].wait()
        partial(snd0, other_off, t)
        ship(1, t)
        ship(0, t)
    for t in range(nt):
        partial(own, own_off, t)
    todo = [(s + LAG * (1 - g), 1 - g, t, s) for g in range(2) for t in range(nt) for s in range(1, 9)]
    for _, q, t, s in sorted(todo, key=lambda e: (e[0], e[2], e[1])):
        stages[s](1 - q, t)
    for cp in sent:
        cp.wait_send()
    for cp in outs:
        cp.wait()


def local(p, normed, out_grad, w_in, hidden_grad, qkv_grad, bucket_order):
    tok, d = normed.shape
    dp, nt, nx, ny, nz = p["dp"], p["t"], p["nx"], p["ny"], p["nz"]
    ch, cy, cz, rows = p["ch"], p["cy"], p["cz"], p["rows"]
    if dp > d:
        normed = jnp.pad(normed, ((0, 0), (0, dp - d)))
        out_grad = jnp.pad(out_grad, ((0, 0), (0, dp - d)))
        w_in = jnp.pad(w_in, ((0, dp - d), (0, 0)))
    total = sum(rows)
    part = (rows[0] // nx, rows[1] // nx)
    per_chunk = 2 + 2 * (nx - 1) + 2 * (ny - 1) + 2 * (nz - 1)
    copies = 2 * nt * per_chunk
    vmem = pl.BlockSpec(memory_space=pltpu.VMEM)
    hbm = pl.BlockSpec(memory_space=pl.ANY)
    gathered = pl.pallas_call(
        functools.partial(kernel, p),
        out_shape=pltpu.VMEM((total, dp), BF16),
        in_specs=[hbm] * 5,
        out_specs=vmem,
        scratch_shapes=[
            pltpu.VMEM((tok, dp), BF16),
            pltpu.VMEM((tok, dp), BF16),
            pltpu.VMEM((p["hw"], dp), BF16),
            pltpu.VMEM((p["hw"], tok), BF16),
            pltpu.VMEM((p["qw"], tok), BF16),
            pltpu.SemaphoreType.DMA((2 * nt + 3,)),
            pltpu.SemaphoreType.DMA((2 * nt,)),
            pltpu.VMEM((total, nt * ch), F32),
            pltpu.VMEM((total, nt * ch), F32),
            pltpu.VMEM((total, nt * ch), F32),
            pltpu.VMEM((total, nt * ch), BF16),
            pltpu.VMEM((part[0], nt * ch), BF16),
            pltpu.VMEM((rows[1], nt * cy), BF16),
            pltpu.VMEM((sum(part), nt * cy), BF16),
            pltpu.VMEM((nx - 1, part[0], nt * ch), BF16),
            pltpu.VMEM((ny - 1, rows[1], nt * cy), BF16),
            pltpu.VMEM((ny - 1, part[0], nt * cy), BF16),
            pltpu.VMEM((nx - 1, part[1], nt * cy), BF16),
            pltpu.VMEM((nz - 1, sum(part), nt * cz), BF16),
            pltpu.VMEM((part[0], nt * ch), F32),
            pltpu.VMEM((rows[1], nt * cy), F32),
            pltpu.VMEM((sum(part), nt * cy), F32),
            pltpu.VMEM((total, dp), BF16),
            pltpu.SemaphoreType.DMA((copies,)),
            pltpu.SemaphoreType.DMA((copies,)),
        ],
        compiler_params=pltpu.CompilerParams(collective_id=0, has_side_effects=True, vmem_limit_bytes=48 * 2**20),
    )(normed, out_grad, w_in.T, hidden_grad.T, qkv_grad.T)
    order = jnp.where(bucket_order < p["qw"], bucket_order, bucket_order + (rows[0] - p["qw"]))
    pick = (order[:, None] == jnp.arange(total, dtype=jnp.int32)[None, :]).astype(BF16)
    return jnp.dot(pick, gathered[:, :d], preferred_element_type=F32).astype(BF16)


def solution(mesh):
    n_row, n_col = mesh.shape["row"], mesh.shape["col"]
    split = P(("row", "col"), None)

    def step(normed, out_grad, w_in, hidden_grad, qkv_grad, bucket_order):
        p = plan(n_row, n_col, normed.shape[1], qkv_grad.shape[1], w_in.shape[1])
        body = jax.shard_map(
            functools.partial(local, p),
            mesh=mesh,
            in_specs=(split, split, P(), split, split, P()),
            out_specs=P(),
            check_vma=False,
        )
        return body(normed, out_grad, w_in, hidden_grad, qkv_grad, bucket_order)

    return step
```

```python
import functools

import jax
import jax.numpy as jnp
from jax import lax
from jax.experimental import pallas as pl
from jax.experimental.pallas import tpu as pltpu
from jax.sharding import PartitionSpec as P

MESH = pl.DeviceIdType.MESH
LAG = 0
F32, BF16 = jnp.float32, jnp.bfloat16


def round_up(a, b):
    return -(-a // b) * b


def plan(n_row, n_col, d, qw, hw):
    nx, nz = n_row // 2, 4
    ny = n_col // nz
    unit = 2 * ny * nz * 128
    dp = round_up(d, unit)
    chunks = dp // unit
    rows = (round_up(qw, 16 * nx), round_up(2 * hw, 16 * nx))
    return dict(nx=nx, ny=ny, nz=nz, dp=dp, t=chunks, rows=rows, ch=ny * nz * 128, cy=nz * 128, cz=128, qw=qw, hw=hw)


def kernel(p, normed, out_grad, w_hbm, hidden_hbm, qkv_hbm, out, nrm, ogr, w_in, hidden_grad, qkv_grad, in_sem, out_sem, own, snd0, rcv0, s1, s2q, s2m, s3, ra_q, ra_m, rb_q, rb_m, rc, acc_q, acc_m, acc2, obuf, ssem, rsem):
    nx, ny, nz, nt = p["nx"], p["ny"], p["nz"], p["t"]
    ch, cy, cz = p["ch"], p["cy"], p["cz"]
    qw, hw = p["qw"], p["hw"]
    rows = p["rows"]
    base = (0, rows[0])
    part = (rows[0] // nx, rows[1] // nx)
    ct = 2 * ch
    r, c = lax.axis_index("row"), lax.axis_index("col")
    ic, ix = lax.rem(r, 2), r // 2
    iy, iz = lax.rem(c, ny), c // ny
    partner = (ix * 2 + (1 - ic), c)
    xp = [(lax.rem(ix + d, nx) * 2 + ic, c) for d in range(nx)]
    yp = [(r, iz * ny + lax.rem(iy + d, ny)) for d in range(ny)]
    zp = [(r, lax.rem(iz + d, nz) * ny + iy) for d in range(nz)]

    loads = {}

    def load(key, src, dst):
        loads[key] = pltpu.make_async_copy(src, dst, in_sem.at[len(loads)])
        loads[key].start()

    def load_cols(name, src, dst, t):
        cols = pl.ds(t * ct, ct)
        load((name, t), src.at[:, cols], dst.at[:, cols])

    load("w", w_hbm, w_in)
    for t in range(nt):
        load_cols("n", normed, nrm, t)
    load("h", hidden_hbm, hidden_grad)
    load("q", qkv_hbm, qkv_grad)
    barrier = pltpu.get_barrier_semaphore()
    peers = [partner] + xp[1:] + yp[1:] + zp[1:]
    for dev in peers:
        pl.semaphore_signal(barrier, inc=1, device_id=dev, device_id_type=MESH)


    sent = []

    def send(src, dst, dev):
        i = len(sent)
        cp = pltpu.make_async_remote_copy(src_ref=src, dst_ref=dst, send_sem=ssem.at[i], recv_sem=rsem.at[i], device_id=dev, device_id_type=MESH)
        cp.start()
        sent.append(cp)
        return cp

    def m(v, k):
        return pl.multiple_of(v, k)

    other_off = m((1 - ic) * ch, 128)
    own_off = m(ic * ch, 128)
    flight = {}

    def dot(lhs, buf, off):
        return jnp.dot(lhs, buf[:, pl.ds(off, ch)], preferred_element_type=F32)

    def zero_tail(g, used, dst, cols):
        if rows[g] > used:
            dst[pl.ds(base[g] + used, rows[g] - used), cols] = jnp.zeros((rows[g] - used, ch), dst.dtype)

    def ship(g, t):
        region = (pl.ds(base[g], rows[g]), pl.ds(t * ch, ch))
        flight[g, t, 0] = [send(snd0.at[region], rcv0.at[region], partner)]

    def partial(dst, off, t):
        cols = pl.ds(t * ch, ch)
        at = m(t * ct + off, 128)
        v = dot(lhs_n, nrm, at)
        dst[pl.ds(0, qw), cols] = v[:qw].astype(dst.dtype)
        dst[pl.ds(base[1], hw), cols] = v[qw:].astype(dst.dtype)
        dst[pl.ds(base[1] + hw, hw), cols] = dot(lhs_out, ogr, at).astype(dst.dtype)
        zero_tail(0, qw, dst, cols)
        zero_tail(1, 2 * hw, dst, cols)

    def wait(g, t, s):
        for cp in flight[g, t, s]:
            cp.wait_recv()

    def row_part(g, i):
        return pl.ds(m(i * part[g], 16), part[g])

    def stage1(g, t):
        wait(g, t, 0)
        region = (pl.ds(base[g], rows[g]), pl.ds(t * ch, ch))
        v = own[region] + rcv0[region].astype(F32)
        own[region] = v
        s1[region] = v.astype(BF16)
        cps = []
        if g == 0:
            for d in range(1, nx):
                src = s1.at[row_part(0, lax.rem(ix + d, nx)), pl.ds(t * ch, ch)]
                cps.append(send(src, ra_q.at[d - 1, :, pl.ds(t * ch, ch)], xp[d]))
        else:
            for d in range(1, ny):
                src = s1.at[pl.ds(base[1], rows[1]), pl.ds(m(t * ch + lax.rem(iy + d, ny) * cy, 128), cy)]
                cps.append(send(src, ra_m.at[d - 1, :, pl.ds(t * cy, cy)], yp[d]))
        flight[g, t, 1] = cps

    def stage2(g, t):
        wait(g, t, 1)
        cps = []
        if g == 0:
            cols = pl.ds(t * ch, ch)
            v = own[row_part(0, ix), cols]
            for d in range(1, nx):
                v = v + ra_q[d - 1, :, cols].astype(F32)
            acc_q[:, cols] = v
            s2q[:, cols] = v.astype(BF16)
            for d in range(1, ny):
                src = s2q.at[:, pl.ds(m(t * ch + lax.rem(iy + d, ny) * cy, 128), cy)]
                cps.append(send(src, rb_q.at[d - 1, :, pl.ds(t * cy, cy)], yp[d]))
        else:
            cols = pl.ds(t * cy, cy)
            v = own[pl.ds(base[1], rows[1]), pl.ds(m(t * ch + iy * cy, 128), cy)]
            for d in range(1, ny):
                v = v + ra_m[d - 1, :, cols].astype(F32)
            acc_m[:, cols] = v
            s2m[:, cols] = v.astype(BF16)
            for d in range(1, nx):
                src = s2m.at[row_part(1, lax.rem(ix + d, nx)), cols]
                cps.append(send(src, rb_m.at[d - 1, :, cols], xp[d]))
        flight[g, t, 2] = cps

    def stage3(g, t):
        wait(g, t, 2)
        cols = pl.ds(t * cy, cy)
        at = pl.ds(g * part[0], part[g])
        if g == 0:
            v = acc_q[:, pl.ds(m(t * ch + iy * cy, 128), cy)]
            for d in range(1, ny):
                v = v + rb_q[d - 1, :, cols].astype(F32)
        else:
            v = acc_m[row_part(1, ix), cols]
            for d in range(1, nx):
                v = v + rb_m[d - 1, :, cols].astype(F32)
        acc2[at, cols] = v
        s3[at, cols] = v.astype(BF16)
        cps = []
        for d in range(1, nz):
            src = s3.at[at, pl.ds(m(t * cy + lax.rem(iz + d, nz) * cz, 128), cz)]
            cps.append(send(src, rc.at[d - 1, at, pl.ds(t * cz, cz)], zp[d]))
        flight[g, t, 3] = cps

    def mine(g):
        return pl.ds(m(base[g] + ix * part[g], 16), part[g])

    def spread(region, devs):
        return [send(obuf.at[region], obuf.at[region], dev) for dev in devs]

    def stage4(g, t):
        wait(g, t, 3)
        at = pl.ds(g * part[0], part[g])
        v = acc2[at, pl.ds(m(t * cy + iz * cz, 128), cz)]
        for d in range(1, nz):
            v = v + rc[d - 1, at, pl.ds(t * cz, cz)].astype(F32)
        region = (mine(g), pl.ds(m(t * ct + own_off + iy * cy + iz * cz, 128), cz))
        obuf[region] = v.astype(BF16)
        flight[g, t, 4] = spread(region, zp[1:])

    def stage5(g, t):
        wait(g, t, 4)
        region = (mine(g), pl.ds(m(t * ct + own_off + iy * cy, 128), cy))
        flight[g, t, 5] = spread(region, (yp if g == 0 else xp)[1:])

    def stage6(g, t):
        wait(g, t, 5)
        if g == 0:
            flight[g, t, 6] = spread((mine(0), pl.ds(m(t * ct + own_off, 128), ch)), xp[1:])
        else:
            flight[g, t, 6] = spread((pl.ds(base[1], rows[1]), pl.ds(m(t * ct + own_off + iy * cy, 128), cy)), yp[1:])

    def stage7(g, t):
        wait(g, t, 6)
        flight[g, t, 7] = spread((pl.ds(base[g], rows[g]), pl.ds(m(t * ct + own_off, 128), ch)), [partner])

    outs = []

    def stage8(g, t):
        wait(g, t, 7)
        region = (pl.ds(base[g], rows[g]), pl.ds(t * ct, ct))
        cp = pltpu.make_async_copy(obuf.at[region], out.at[region], out_sem.at[g * nt + t])
        cp.start()
        outs.append(cp)

    stages = [None, stage1, stage2, stage3, stage4, stage5, stage6, stage7, stage8]

    pre = None
    for t in range(nt):
        loads["n", t].wait()
        if t == 0:
            loads["w"].wait()
        load_cols("o", out_grad, ogr, t)
        cols = slice(t * ct, (t + 1) * ct)
        term = lax.dot_general(w_in[:, cols], nrm[:, cols], (((1,), (1,)), ((), ())), preferred_element_type=F32)
        pre = term if pre is None else pre + term
    loads["h"].wait()
    loads["q"].wait()
    lhs_q = qkv_grad[...]
    cdf = 0.5 * (1.0 + lax.erf(pre * 0.7071067811865476))
    pdf = jnp.exp(-0.5 * pre * pre) * 0.3989422804014327
    lhs_out = (pre * cdf).astype(BF16)
    lhs_in = (hidden_grad[...].astype(F32) * (cdf + pre * pdf)).astype(BF16)
    lhs_n = jnp.concatenate([lhs_q, lhs_in], axis=0)
    pl.semaphore_wait(barrier, len(peers))
    for t in range(nt):
        loads["o", t].wait()
        partial(snd0, other_off, t)
        ship(1, t)
        ship(0, t)
    for t in range(nt):
        partial(own, own_off, t)
    todo = [(s + LAG * (1 - g), 1 - g, t, s) for g in range(2) for t in range(nt) for s in range(1, 9)]
    for _, q, t, s in sorted(todo, key=lambda e: (e[0], e[2], e[1])):
        stages[s](1 - q, t)
    for cp in sent:
        cp.wait_send()
    for cp in outs:
        cp.wait()


def local(p, normed, out_grad, w_in, hidden_grad, qkv_grad, bucket_order):
    tok, d = normed.shape
    dp, nt, nx, ny, nz = p["dp"], p["t"], p["nx"], p["ny"], p["nz"]
    ch, cy, cz, rows = p["ch"], p["cy"], p["cz"], p["rows"]
    if dp > d:
        normed = jnp.pad(normed, ((0, 0), (0, dp - d)))
        out_grad = jnp.pad(out_grad, ((0, 0), (0, dp - d)))
        w_in = jnp.pad(w_in, ((0, dp - d), (0, 0)))
    total = sum(rows)
    part = (rows[0] // nx, rows[1] // nx)
    per_chunk = 2 + 2 * (nx - 1) + 2 * (ny - 1) + 2 * (nz - 1)
    copies = 2 * nt * per_chunk
    vmem = pl.BlockSpec(memory_space=pltpu.VMEM)
    hbm = pl.BlockSpec(memory_space=pl.ANY)
    gathered = pl.pallas_call(
        functools.partial(kernel, p),
        out_shape=pltpu.VMEM((total, dp), BF16),
        in_specs=[hbm] * 5,
        out_specs=vmem,
        scratch_shapes=[
            pltpu.VMEM((tok, dp), BF16),
            pltpu.VMEM((tok, dp), BF16),
            pltpu.VMEM((p["hw"], dp), BF16),
            pltpu.VMEM((p["hw"], tok), BF16),
            pltpu.VMEM((p["qw"], tok), BF16),
            pltpu.SemaphoreType.DMA((2 * nt + 3,)),
            pltpu.SemaphoreType.DMA((2 * nt,)),
            pltpu.VMEM((total, nt * ch), F32),
            pltpu.VMEM((total, nt * ch), BF16),
            pltpu.VMEM((total, nt * ch), BF16),
            pltpu.VMEM((total, nt * ch), BF16),
            pltpu.VMEM((part[0], nt * ch), BF16),
            pltpu.VMEM((rows[1], nt * cy), BF16),
            pltpu.VMEM((sum(part), nt * cy), BF16),
            pltpu.VMEM((nx - 1, part[0], nt * ch), BF16),
            pltpu.VMEM((ny - 1, rows[1], nt * cy), BF16),
            pltpu.VMEM((ny - 1, part[0], nt * cy), BF16),
            pltpu.VMEM((nx - 1, part[1], nt * cy), BF16),
            pltpu.VMEM((nz - 1, sum(part), nt * cz), BF16),
            pltpu.VMEM((part[0], nt * ch), F32),
            pltpu.VMEM((rows[1], nt * cy), F32),
            pltpu.VMEM((sum(part), nt * cy), F32),
            pltpu.VMEM((total, dp), BF16),
            pltpu.SemaphoreType.DMA((copies,)),
            pltpu.SemaphoreType.DMA((copies,)),
        ],
        compiler_params=pltpu.CompilerParams(collective_id=0, has_side_effects=True, vmem_limit_bytes=67043328 - 4 * total * dp),
    )(normed, out_grad, w_in.T, hidden_grad.T, qkv_grad.T)
    order = jnp.where(bucket_order < p["qw"], bucket_order, bucket_order + (rows[0] - p["qw"]))
    pick = (order[:, None] == jnp.arange(total, dtype=jnp.int32)[None, :]).astype(BF16)
    return jnp.dot(pick, gathered[:, :d], preferred_element_type=F32).astype(BF16)


def solution(mesh):
    n_row, n_col = mesh.shape["row"], mesh.shape["col"]
    split = P(("row", "col"), None)

    def step(normed, out_grad, w_in, hidden_grad, qkv_grad, bucket_order):
        p = plan(n_row, n_col, normed.shape[1], qkv_grad.shape[1], w_in.shape[1])
        body = jax.shard_map(
            functools.partial(local, p),
            mesh=mesh,
            in_specs=(split, split, P(), split, split, P()),
            out_specs=P(),
            check_vma=False,
        )
        return body(normed, out_grad, w_in, hidden_grad, qkv_grad, bucket_order)

    return step
```
